256 devices in a mesh: tm: 8 (over y, z_hi), height: 32 (over z_lo, x, core).
Axes of the slice: x: 4, y: 4, z: 8 (z_hi: 2, z_lo: 4; z = z_hi * 4 + z_lo), core: 2. Of those that a mesh axis runs over, the one named last changes fastest.
Arguments:
- latents: bfloat16 [2, 16, 64, 128, 512], P(None, 'tm', 'height'), may hold values from -6 to 6
- norm_gain: float32 [512], replicated, may hold values from 0.25 to 1.75
- spatial_weight: bfloat16 [3, 3, 512, 512], replicated, may hold values from -0.09375 to 0.09375
- temporal_weight: float32 [3, 512], replicated, may hold values from -3 to 3
- codebooks: bfloat16 [2, 65536, 512], P(None, 'height'), may hold values from -6 to 6
- ema_counts: float32 [2, 65536], P(None, 'height'), may hold values from 0.3 to 30
- ema_sums: float32 [2, 65536, 512], P(None, 'height', 'tm'), may hold values from -6 to 6
- decay: float32 [2], replicated, may hold values from 0.6 to 0.9
- codes_first: int32 [2, 16, 64, 128], P(None, 'tm', 'height'), may hold values from 0 to 65535, as said below
- codes_second: int32 [2, 16, 64, 128], P(None, 'tm', 'height'), may hold values from 0 to 65535, as said below
Outputs:
- ema_counts_new: float32 [2, 65536], P(None, 'height')
- ema_sums_new: float32 [2, 65536, 512], P(None, 'height', 'tm')
- error: float32 [2, 16, 64, 128], P(None, 'tm', 'height')
The draws below stay inside these ranges and needn't reach their ends.
Inputs may be any that keep to these rules, and one draw needn't show every extreme that they name: `codes_first`: the codes of index o of height are o * 2048 to (o + 1) * 2048 - 1. In the latents of one device (all 2 clips over its 2 frames and 2 rows) at most 64 name codes of one owner o, and in every draw, for every index of tm, some owner gets exactly 64 from every device of that index. `codes_second`: as for codes_first, drawn independently.
All inputs are finite; a program needn't handle non-finite values.
Results may differ from the reference program's by a relative error of at most 0.0031.
Values may be sent and summed in bfloat16 or wider, within the bound.
No kernel may reach another device: no remote copies, remote signals or barrier semaphores. Data moves between devices by JAX's collectives and lax.ppermute only.
A program may use at most 128 MiB of HBM per device.

```python
import math
import jax
import jax.numpy as jnp
from jax import lax

C = 512
CODE_DEV = 2048
CLIPS = 2
TF_DEV = 2
ROWS_DEV = 2
WIDTH = 128
FRAMES = 16
HEIGHT = 64
CODES = 65536


def owner_codes(key, salt):
    key = jax.random.fold_in(key, salt)
    slab_count = FRAMES // TF_DEV
    band_count = HEIGHT // ROWS_DEV
    per_block = CLIPS * TF_DEV * ROWS_DEV * WIDTH
    capacity = 2 * per_block // band_count
    slot_total = band_count * capacity
    subkeys = jax.random.split(key, 5)
    heat_level = jax.random.randint(subkeys[0], (slab_count, band_count, band_count), 0, 3)
    hottest = jax.random.randint(subkeys[1], (slab_count,), 0, band_count)
    heat_level = jnp.where(jnp.arange(band_count)[None, None, :] == hottest[:, None, None], 4, heat_level)
    slot_owner = jnp.arange(slot_total) // capacity
    orders = jax.vmap(lambda subkey: jax.random.permutation(subkey, slot_total))(jax.random.split(subkeys[2], slab_count * band_count)).reshape(slab_count, band_count, slot_total)
    scores = heat_level[:, :, slot_owner] * slot_total + orders
    chosen = jnp.argsort(-scores, axis=-1, stable=True)[:, :, :per_block]
    owners = chosen // capacity
    shuffles = jax.vmap(lambda subkey: jax.random.permutation(subkey, per_block))(jax.random.split(subkeys[3], slab_count * band_count)).reshape(slab_count, band_count, per_block)
    owners = jnp.take_along_axis(owners, shuffles, axis=-1)
    within = jax.random.randint(subkeys[4], (slab_count, band_count, per_block), 0, CODE_DEV)
    codes = owners * CODE_DEV + within
    codes = codes.reshape(slab_count, band_count, CLIPS, TF_DEV, ROWS_DEV, WIDTH)
    codes = codes.transpose(2, 0, 3, 1, 4, 5).reshape(CLIPS, FRAMES, HEIGHT, WIDTH)
    return codes.astype(jnp.int32)


def draw_codes_first(key, part):
    return owner_codes(key, 11)


def draw_codes_second(key, part):
    return owner_codes(key, 23)


def shard_levels(stream_key, extent, cuts, low, high):
    level = 1.0
    for dim, parts in cuts:
        heights = jax.random.uniform(jax.random.fold_in(jax.random.fold_in(stream_key, 6), dim), (parts,), jnp.float32, low / len(cuts), high / len(cuts))
        level = level * jnp.repeat(jnp.exp(heights), extent[dim] // parts).reshape((-1,) + (1,) * (len(extent) - 1 - dim))
    return level


def centred(own_key, shape, spread, limit, pieces=(), dtype=jnp.bfloat16):
    level = shard_levels(own_key, shape, pieces, -0.22, 0.18) if pieces else 1.0
    values = jax.random.normal(own_key, shape, jnp.float32) * spread * level
    return jnp.minimum(jnp.maximum(values, -limit), limit).astype(dtype)


def setup_inputs(seed: int = 0) -> dict:
    arg_keys = jax.random.split(jax.random.key(seed), 11)
    return {
        "latents": centred(arg_keys[0], (CLIPS, FRAMES, HEIGHT, WIDTH, C), 1.0, 6.0, ((1, 8), (2, 32))),
        "norm_gain": jnp.clip(1.0 + 0.15 * jax.random.normal(arg_keys[1], (C,), jnp.float32), 0.25, 1.75),
        "spatial_weight": centred(arg_keys[2], (3, 3, C, C), (9 * C) ** -0.5, 0.09375),
        "temporal_weight": centred(arg_keys[3], (3, C), 0.6, 3.0, (), jnp.float32),
        "codebooks": centred(arg_keys[4], (2, CODES, C), 1.0, 6.0, ((1, 32),)),
        "ema_counts": jnp.clip(jnp.exp(math.log(30.0) - 4.6051701 * jax.random.uniform(arg_keys[5], (2, CODES), jnp.float32) ** shard_levels(arg_keys[5], (2, CODES), ((1, 32),), -0.2, 0.2)), 0.3, 30.0),
        "ema_sums": centred(arg_keys[6], (2, CODES, C), 1.0, 6.0, ((1, 32), (2, 8)), jnp.float32),
        "decay": jnp.clip(jax.random.uniform(arg_keys[7], (2,), jnp.float32, 0.6, 0.9), 0.6, 0.9),
        "codes_first": draw_codes_first(jax.random.fold_in(arg_keys[10], 71), 0),
        "codes_second": draw_codes_second(jax.random.fold_in(arg_keys[10], 71), 0),
    }


def reference(latents, norm_gain, spatial_weight, temporal_weight, codebooks, ema_counts, ema_sums, decay, codes_first, codes_second):
    widened = latents.astype(jnp.float32)
    inverse = lax.rsqrt(lax.optimization_barrier(jnp.mean(widened * widened, axis=-1, keepdims=True)) + 1e-06)
    normed = (widened * inverse * norm_gain).astype(jnp.bfloat16)
    frame_stack = normed.reshape(CLIPS * FRAMES, HEIGHT, WIDTH, C)

    def convolve(frame):
        padded = jnp.pad(frame, ((1, 1), (1, 1), (0, 0)))
        summed = jnp.zeros((HEIGHT * WIDTH, C), jnp.float32)
        for row_tap in range(3):
            for col_tap in range(3):
                window = padded[row_tap:row_tap + HEIGHT, col_tap:col_tap + WIDTH].reshape(-1, C)
                summed = summed + jnp.dot(window, spatial_weight[row_tap, col_tap], preferred_element_type=jnp.float32)
        return jax.nn.silu(summed).astype(jnp.bfloat16).reshape(HEIGHT, WIDTH, C)
    hidden = lax.map(convolve, frame_stack).reshape(CLIPS, FRAMES, HEIGHT, WIDTH, C)
    delayed = jnp.pad(hidden, ((0, 0), (2, 0), (0, 0), (0, 0), (0, 0)))
    mixed = jnp.zeros(latents.shape, jnp.float32)
    for tap in range(3):
        mixed = mixed + temporal_weight[tap] * delayed[:, tap:tap + FRAMES].astype(jnp.float32)
    encoded = (widened + mixed).astype(jnp.bfloat16)
    flat = encoded.reshape(-1, C)
    first_ids = codes_first.reshape(-1)
    second_ids = codes_second.reshape(-1)
    first_quant = jnp.take(codebooks[0], first_ids, axis=0)
    residual = (flat.astype(jnp.float32) - first_quant.astype(jnp.float32)).astype(jnp.bfloat16)
    second_quant = jnp.take(codebooks[1], second_ids, axis=0)
    leftover = residual.astype(jnp.float32) - second_quant.astype(jnp.float32)
    error = lax.optimization_barrier(jnp.mean(leftover * leftover, axis=-1)).reshape(codes_first.shape)
    unit = jnp.ones(first_ids.shape, jnp.float32)
    counts = jnp.stack([jax.ops.segment_sum(unit, first_ids, num_segments=CODES), jax.ops.segment_sum(unit, second_ids, num_segments=CODES)])
    sums = jnp.stack([jax.ops.segment_sum(flat.astype(jnp.float32), first_ids, num_segments=CODES), jax.ops.segment_sum(residual.astype(jnp.float32), second_ids, num_segments=CODES)])
    keep = decay[:, None]
    ema_counts_new = keep * ema_counts + (1.0 - keep) * counts
    ema_sums_new = decay[:, None, None] * ema_sums + (1.0 - decay[:, None, None]) * sums
    return (ema_counts_new, ema_sums_new, error)
```

```python
import functools

import jax
import jax.numpy as jnp
from jax import lax
from jax.experimental import pallas as pl
from jax.experimental.pallas import tpu as pltpu
from jax.sharding import PartitionSpec as P

BOTH = ("tm", "height")
OWNERS = 32
SLABS = 8
CAP = 64
HALF = CAP // 2
ROWS = 1024
CH = 512
CHUNK = CH // SLABS
CODE_ROWS = 2048
VMEM_LIMIT = 56 * 1024 * 1024
NT = (((1,), (1,)), ((), ()))
F32 = jnp.float32
BF16 = jnp.bfloat16


def iota(shape, dim):
    return lax.broadcasted_iota(jnp.int32, shape, dim)


def params(*semantics):
    return pltpu.CompilerParams(
        vmem_limit_bytes=VMEM_LIMIT, dimension_semantics=semantics or None
    )


def cost(flops, moved):
    return pl.CostEstimate(flops=flops, transcendentals=0, bytes_accessed=moved)


def plan_kernel(codes_ref, ids_ref, slot_ref, place_ref):
    tri = (iota((ROWS, ROWS), 0) < iota((ROWS, ROWS), 1)).astype(F32).astype(BF16)
    table = jnp.zeros((3 * OWNERS, 2 * CAP), F32)
    for sec in range(2):
        code = codes_ref[sec : sec + 1, :]
        owner = code >> 11
        local = code & (CODE_ROWS - 1)
        hot = (iota((OWNERS, ROWS), 0) == owner).astype(F32)
        ahead = jnp.dot(hot.astype(BF16), tri, preferred_element_type=F32)
        rank = jnp.sum(hot * ahead, axis=0, keepdims=True).astype(jnp.int32)
        slot_ref[sec : sec + 1, :] = owner * CAP + rank
        place_ref[sec : sec + 1, :] = (
            (rank >> 5) * (OWNERS * HALF) + owner * HALF + (rank & (HALF - 1))
        )
        high = (local >> 6).astype(F32)
        low = (local & 63).astype(F32)
        left = jnp.concatenate([hot, hot * high, hot * low], axis=0).astype(BF16)
        right = (iota((2 * CAP, ROWS), 0) == rank + sec * CAP).astype(F32).astype(BF16)
        table = table + lax.dot_general(left, right, NT, preferred_element_type=F32)
    filled = table[:OWNERS]
    value = table[OWNERS : 2 * OWNERS] * 64.0 + table[2 * OWNERS :]
    ids_ref[...] = jnp.where(filled > 0.5, value, -1.0).astype(jnp.int32)


def make_plan(codes):
    return pl.pallas_call(
        plan_kernel,
        out_shape=(
            jax.ShapeDtypeStruct((OWNERS, 2 * CAP), jnp.int32),
            jax.ShapeDtypeStruct((2, ROWS), jnp.int32),
            jax.ShapeDtypeStruct((2, ROWS), jnp.int32),
        ),
        compiler_params=params(),
        cost_estimate=cost(4 * OWNERS * ROWS * ROWS, 1 << 16),
        name="plan",
    )(codes)


def columns(row):
    parts = []
    for start in range(0, row.shape[1], 128):
        piece = jnp.broadcast_to(row[:, start : start + 128], (128, 128))
        parts.append(jnp.transpose(piece))
    return jnp.concatenate(parts, axis=0)


def one_hot(cols, width, offset=0):
    lanes = iota(cols.shape, 1)
    parts = [
        (cols == lanes + (offset + start)).astype(F32).astype(BF16)
        for start in range(0, width, 128)
    ]
    return jnp.concatenate(parts, axis=1)


def serve_kernel(ids_ref, table_ref, out_ref):
    picks = one_hot(columns(ids_ref[0]), CODE_ROWS)
    got = jnp.dot(picks, table_ref[0], preferred_element_type=F32)
    out_ref[...] = got.astype(BF16).reshape(out_ref.shape)


def serve(ids, codebooks, sec):
    step = 512
    return pl.pallas_call(
        serve_kernel,
        grid=(ROWS // step,),
        in_specs=[
            pl.BlockSpec((1, 1, step), lambda i: (i, 0, 0)),
            pl.BlockSpec((1, CODE_ROWS, CH), lambda i: (sec, 0, 0)),
        ],
        out_specs=pl.BlockSpec((step // HALF, HALF, CH), lambda i: (i, 0, 0)),
        out_shape=jax.ShapeDtypeStruct((OWNERS, HALF, CH), BF16),
        compiler_params=params("arbitrary"),
        cost_estimate=cost(2 * ROWS * CODE_ROWS * CH, 3 << 20),
        name="serve",
    )(ids.reshape(ROWS // step, 1, step), codebooks)


def picked(place_row, near_ref, far_ref):
    cols = columns(place_row)
    size = OWNERS * HALF
    got = jnp.dot(
        one_hot(cols, size), near_ref[...].reshape(size, CH), preferred_element_type=F32
    )
    return got + jnp.dot(
        one_hot(cols, size, size), far_ref[...].reshape(size, CH), preferred_element_type=F32
    )


def unpack_kernel(place_ref, near_ref, far_ref, out_ref):
    out_ref[...] = picked(place_ref[0], near_ref, far_ref).astype(BF16)


def unpack(place, near, far):
    step = 512
    whole = pl.BlockSpec((OWNERS, HALF, CH), lambda i: (0, 0, 0))
    return pl.pallas_call(
        unpack_kernel,
        grid=(ROWS // step,),
        in_specs=[pl.BlockSpec((1, 1, step), lambda i: (i, 0, 0)), whole, whole],
        out_specs=pl.BlockSpec((step, CH), lambda i: (i, 0)),
        out_shape=jax.ShapeDtypeStruct((ROWS, CH), BF16),
        compiler_params=params("arbitrary"),
        cost_estimate=cost(2 * ROWS * CODE_ROWS * CH, 3 << 20),
        name="unpack",
    )(place.reshape(ROWS // step, 1, step), near, far)


def conv_kernel(before_ref, own_ref, after_ref, gain_ref, weight_ref, out_ref, normed_ref):
    @pl.when(pl.program_id(0) == 0)
    def _():
        def put(values, start):
            wide = values.astype(F32)
            inverse = lax.rsqrt(jnp.mean(wide * wide, axis=-1, keepdims=True) + 1e-06)
            normed_ref[:, start : start + values.shape[1], :] = (
                wide * inverse * gain_ref[...]
            ).astype(BF16)

        put(own_ref[...], 128)
        put(before_ref[...], 0)
        put(after_ref[...], 384)

    frames = normed_ref.shape[0]
    width = out_ref.shape[-1]
    column = iota((frames * 256, width), 0) & 127
    total = None
    for col in (1, 0, 2):
        part = None
        for row in range(3):
            window = normed_ref[:, row * 128 : row * 128 + 256, :].reshape(frames * 256, CH)
            made = jnp.dot(window, weight_ref[row, col], preferred_element_type=F32)
            part = made if part is None else part + made
        if col == 0:
            part = jnp.where(column == 0, 0.0, pltpu.roll(part, 1, 0))
        elif col == 2:
            part = jnp.where(column == 127, 0.0, pltpu.roll(part, frames * 256 - 1, 0))
        total = part if total is None else total + part
    out_ref[...] = (total / (1.0 + jnp.exp(-total))).astype(BF16).reshape(out_ref.shape)


def convolve(before, own, after, gain, weight):
    width = 256
    frames = own.shape[0]
    whole = lambda rows: pl.BlockSpec((frames, rows, CH), lambda i: (0, 0, 0))
    return pl.pallas_call(
        conv_kernel,
        grid=(CH // width,),
        in_specs=[
            whole(128),
            whole(256),
            whole(128),
            pl.BlockSpec((1, 1, CH), lambda i: (0, 0, 0)),
            pl.BlockSpec((3, 3, CH, width), lambda i: (0, 0, 0, i)),
        ],
        out_specs=pl.BlockSpec((frames, 256, width), lambda i: (0, 0, i)),
        out_shape=jax.ShapeDtypeStruct((frames, 256, CH), BF16),
        scratch_shapes=[pltpu.VMEM((frames, 512, CH), BF16)],
        compiler_params=params("arbitrary"),
        cost_estimate=cost(18 * ROWS * CH * CH, 8 << 20),
        name="conv",
    )(before, own, after, gain.reshape(1, 1, CH), weight)


def pack_into(turned_ref, slot_row, out_ref):
    step = 256
    left = iota((SLABS, HALF, 128), 2) < 64

    def chunk(index, carry):
        hot = (iota((step, ROWS), 0) + index * step == slot_row).astype(F32).astype(BF16)
        block = lax.dot_general(turned_ref[...], hot, NT, preferred_element_type=F32)
        for pair in range(step // 128):
            piece = block[:, pair * 128 : (pair + 1) * 128].reshape(SLABS, CHUNK, 128)
            top, low = piece[:, :HALF], piece[:, HALF:]
            owner = index * (step // CAP) + 2 * pair
            out_ref[:, owner] = jnp.where(left, top, pltpu.roll(low, 64, 2)).astype(BF16)
            out_ref[:, owner + 1] = jnp.where(left, pltpu.roll(top, 64, 2), low).astype(BF16)
        return carry

    lax.fori_loop(0, OWNERS * CAP // step, chunk, 0)


MESSAGE = jax.ShapeDtypeStruct((SLABS, OWNERS, HALF, 128), BF16)


def first_kernel(lat_ref, hid_ref, prev_ref, taps_ref, slot_ref, out_ref, enc_ref, turned_ref):
    taps = [taps_ref[tap : tap + 1, :] for tap in range(3)]
    clips, frames = lat_ref.shape[0], lat_ref.shape[1]
    for clip in range(clips):
        series = [prev_ref[clip, f].astype(F32) for f in range(frames)]
        series += [hid_ref[clip, f].astype(F32) for f in range(frames)]
        for frame in range(frames):
            mixed = taps[0] * series[frame]
            mixed = mixed + taps[1] * series[frame + 1]
            mixed = mixed + taps[2] * series[frame + 2]
            made = (lat_ref[clip, frame].astype(F32) + mixed).astype(BF16)
            start = (clip * frames + frame) * 256
            enc_ref[start : start + 256, :] = made
            turned_ref[:, start : start + 256] = jnp.transpose(made.astype(F32)).astype(BF16)
    pack_into(turned_ref, slot_ref[...], out_ref)


def pack_first(lat, hid, prev, taps, slot):
    return pl.pallas_call(
        first_kernel,
        out_shape=(MESSAGE, jax.ShapeDtypeStruct((ROWS, CH), BF16)),
        scratch_shapes=[pltpu.VMEM((CH, ROWS), BF16)],
        compiler_params=params(),
        cost_estimate=cost(2 * ROWS * CODE_ROWS * CH, 6 << 20),
        name="pack_first",
    )(lat, hid, prev, taps, slot)


def second_kernel(enc_ref, place_ref, slot_ref, near_ref, far_ref, out_ref, res_ref, turned_ref):
    for start in range(0, ROWS, 512):
        quant = picked(place_ref[:, start : start + 512], near_ref, far_ref)
        made = (enc_ref[start : start + 512, :].astype(F32) - quant).astype(BF16)
        res_ref[start : start + 512, :] = made
        turned_ref[:, start : start + 512] = jnp.transpose(made.astype(F32)).astype(BF16)
    pack_into(turned_ref, slot_ref[...], out_ref)


def pack_second(enc, place, slot, near, far):
    return pl.pallas_call(
        second_kernel,
        out_shape=(MESSAGE, jax.ShapeDtypeStruct((ROWS, CH), BF16)),
        scratch_shapes=[pltpu.VMEM((CH, ROWS), BF16)],
        compiler_params=params(),
        cost_estimate=cost(4 * ROWS * CODE_ROWS * CH, 6 << 20),
        name="pack_second",
    )(enc, place, slot, near, far)


def sums_kernel(sec, got_ref, ids_ref, ema_ref, decay_ref, *rest):
    out_ref, count_ref, acc_ref = rest[-3:]
    step = pl.program_id(0)

    @pl.when(step == 0)
    def _():
        acc_ref[...] = jnp.zeros_like(acc_ref)

    left = iota((HALF, 128), 1) < 64
    groups = CODE_ROWS // CH
    hots, wides = [], []
    for pair in range(got_ref.shape[0] // 2):
        code = ids_ref[0, pair : pair + 1, :]
        group = code >> 9
        hots.append((iota((CH, 128), 0) == (code & (CH - 1))).astype(F32).astype(BF16))
        one = got_ref[2 * pair].astype(F32)
        two = got_ref[2 * pair + 1].astype(F32)
        block = jnp.concatenate(
            [
                jnp.where(left, one, pltpu.roll(two, 64, 1)),
                jnp.where(left, pltpu.roll(one, 64, 1), two),
            ],
            axis=0,
        )
        rows = [jnp.where(group == g, block, 0.0) for g in range(groups)]
        rows.append((iota((8, 128), 0) == group).astype(F32))
        wides.append(jnp.concatenate(rows, axis=0).astype(BF16))
    hot = jnp.concatenate(hots, axis=1)
    wide = jnp.concatenate(wides, axis=1)
    acc_ref[...] += lax.dot_general(wide, hot, NT, preferred_element_type=F32)

    @pl.when(step == pl.num_programs(0) - 1)
    def _():
        keep = decay_ref[sec]
        for g in range(groups):
            span = slice(g * CH, (g + 1) * CH)
            out_ref[0, :, span] = keep * ema_ref[0, :, span] + (1.0 - keep) * acc_ref[
                g * CHUNK : (g + 1) * CHUNK, :
            ]
            count_ref[:, span] = acc_ref[groups * CHUNK + g : groups * CHUNK + g + 1, :]


def sums(sec, got, ids, ema, decay, earlier=None):
    sources = 16
    block = pl.BlockSpec((1, CHUNK, CODE_ROWS), lambda i: (sec, 0, 0))
    in_specs = [
        pl.BlockSpec((sources, HALF, 128), lambda i: (i, 0, 0)),
        pl.BlockSpec((1, sources // 2, 128), lambda i: (i, 0, 0)),
        block,
        pl.BlockSpec(memory_space=pltpu.SMEM),
    ]
    args = [got, ids, ema, decay]
    aliases = {}
    if earlier is not None:
        in_specs.append(pl.BlockSpec(memory_space=pl.ANY))
        args.append(earlier)
        aliases = {4: 0}
    return pl.pallas_call(
        functools.partial(sums_kernel, sec),
        grid=(got.shape[0] // sources,),
        in_specs=in_specs,
        out_specs=(block, pl.BlockSpec((1, CODE_ROWS), lambda i: (0, 0))),
        out_shape=(
            jax.ShapeDtypeStruct((2, CHUNK, CODE_ROWS), F32),
            jax.ShapeDtypeStruct((1, CODE_ROWS), F32),
        ),
        scratch_shapes=[pltpu.VMEM((CODE_ROWS // CH * CHUNK + 8, CH), F32)],
        input_output_aliases=aliases,
        compiler_params=params("arbitrary"),
        cost_estimate=cost(2 * 256 * CH * 256 * CAP, 4 << 20),
        name="sums",
    )(*args)


def runs(shift):
    groups = []
    for y in range(4):
        for which in range(2):
            group = []
            for z_lo in range(4):
                z_hi = which ^ (z_lo >> 1) if shift else which
                first = (y * 2 + z_hi) * OWNERS + z_lo * 8
                group.extend(range(first, first + 8))
            groups.append(group)
    return groups


def run_exchange(x, shift):
    return lax.all_to_all(x, BOTH, 0, 0, axis_index_groups=runs(shift), tiled=True)


def body(
    latents,
    norm_gain,
    spatial_weight,
    temporal_weight,
    codebooks,
    ema_counts,
    ema_sums,
    decay,
    codes_first,
    codes_second,
):
    tm, height = lax.axis_index("tm"), lax.axis_index("height")
    up = [(i, i + 1) for i in range(OWNERS - 1)]
    down = [(i + 1, i) for i in range(OWNERS - 1)]
    before = lax.ppermute(latents[:, :, 1], "height", up).reshape(4, 128, CH)
    after = lax.ppermute(latents[:, :, 0], "height", down).reshape(4, 128, CH)

    codes = jnp.stack([codes_first.reshape(ROWS), codes_second.reshape(ROWS)])
    ids, slot, place = make_plan(codes)
    sent = jnp.broadcast_to(ids[None], (SLABS, OWNERS, 2 * CAP)).reshape(-1, 2 * CAP)
    known = lax.all_to_all(sent, BOTH, 0, 0, tiled=True)
    by_slab = known.reshape(SLABS, OWNERS, 2 * CAP)

    near_ids = lax.dynamic_index_in_dim(by_slab, tm, 0, keepdims=False)
    which = (tm & 1) ^ ((height >> 4) & 1)
    base = tm & ~1
    far_ids = jnp.concatenate(
        [
            lax.dynamic_index_in_dim(by_slab, base + which, 0, keepdims=False)[:16],
            lax.dynamic_index_in_dim(by_slab, base + (1 - which), 0, keepdims=False)[16:],
        ]
    )
    answers = []
    for sec in range(2):
        near = serve(near_ids[:, sec * CAP : sec * CAP + HALF].reshape(ROWS), codebooks, sec)
        near = run_exchange(near, 0)
        far = serve(far_ids[:, sec * CAP + HALF : (sec + 1) * CAP].reshape(ROWS), codebooks, sec)
        far = run_exchange(far, 1)
        answers.append((near, far))

    own = latents.reshape(4, 256, CH)
    hidden = convolve(before, own, after, norm_gain, spatial_weight)
    previous = lax.ppermute(hidden, "tm", [(i, i + 1) for i in range(SLABS - 1)])

    clip_form = lambda x: x.reshape(2, 2, 256, CH)
    first_out, encoded = pack_first(
        clip_form(latents), clip_form(hidden), clip_form(previous), temporal_weight, slot[:1]
    )
    first_in = lax.all_to_all(
        first_out.reshape(-1, HALF, 128), BOTH, 0, 0, tiled=True
    )
    second_out, residual = pack_second(encoded, place[:1], slot[1:], *answers[0])
    second_in = lax.all_to_all(
        second_out.reshape(-1, HALF, 128), BOTH, 0, 0, tiled=True
    )

    second_quant = unpack(place[1], *answers[1])
    leftover = residual.astype(F32) - second_quant.astype(F32)
    error = jnp.mean(leftover * leftover, axis=-1).reshape(codes_first.shape)

    turned_ema = jnp.swapaxes(ema_sums, 1, 2)
    pair_ids = [known[:, sec * CAP : (sec + 1) * CAP].reshape(16, 8, 128) for sec in range(2)]
    partial, counts_first = sums(0, first_in, pair_ids[0], turned_ema, decay)
    done, counts_second = sums(1, second_in, pair_ids[1], turned_ema, decay, partial)
    ema_sums_new = jnp.swapaxes(done, 1, 2)

    counts = jnp.concatenate([counts_first, counts_second])
    keep = decay[:, None]
    ema_counts_new = keep * ema_counts + (1.0 - keep) * counts
    return (ema_counts_new, ema_sums_new, error)


def solution(mesh):
    return jax.shard_map(
        body,
        mesh=mesh,
        in_specs=(
            P(None, "tm", "height", None, None),
            P(),
            P(),
            P(),
            P(None, "height", None),
            P(None, "height"),
            P(None, "height", "tm"),
            P(),
            P(None, "tm", "height", None),
            P(None, "tm", "height", None),
        ),
        out_specs=(P(None, "height"), P(None, "height", "tm"), P(None, "tm", "height", None)),
        check_vma=False,
    )
```

```python
import functools

import jax
import jax.numpy as jnp
from jax import lax
from jax.experimental import pallas as pl
from jax.experimental.pallas import tpu as pltpu
from jax.sharding import PartitionSpec as P


BOTH = ("tm", "height")
OWNERS = 32
SLABS = 8
CAP = 64
HALF = CAP // 2
PLANE = 8
ROWS = 1024
CH = 512
CHUNK = CH // SLABS
CODE_ROWS = 2048
VMEM_LIMIT = 56 * 1024 * 1024
NT = (((1,), (1,)), ((), ()))
F32 = jnp.float32
BF16 = jnp.bfloat16


def iota(shape, dim):
    return lax.broadcasted_iota(jnp.int32, shape, dim)


def params(*semantics):
    return pltpu.CompilerParams(
        vmem_limit_bytes=VMEM_LIMIT, dimension_semantics=semantics or None
    )


def cost(flops, moved):
    return pl.CostEstimate(flops=flops, transcendentals=0, bytes_accessed=moved)


def plan_kernel(z_ref, codes_ref, ids_ref, slot_ref, place_ref):
    tri = (iota((ROWS, ROWS), 0) < iota((ROWS, ROWS), 1)).astype(F32).astype(BF16)
    table = jnp.zeros((3 * OWNERS, 2 * CAP), F32)
    for sec in range(2):
        code = codes_ref[sec : sec + 1, :]
        owner = code >> 11
        local = code & (CODE_ROWS - 1)
        hot = (iota((OWNERS, ROWS), 0) == owner).astype(F32)
        ahead = jnp.dot(hot.astype(BF16), tri, preferred_element_type=F32)
        rank = jnp.sum(hot * ahead, axis=0, keepdims=True).astype(jnp.int32)
        slot_ref[sec : sec + 1, :] = owner * CAP + rank
        away = ((owner >> 3) - z_ref[0]) & 3
        inner = owner & 7
        full = jnp.where(away == 0, 0, jnp.where(away == 3, PLANE * CAP, 2 * PLANE * CAP))
        split = 3 * PLANE * CAP + (rank >> 5) * (PLANE * HALF) + inner * HALF + (rank & (HALF - 1))
        place_ref[sec : sec + 1, :] = jnp.where(away == 2, split, full + inner * CAP + rank)
        high = (local >> 6).astype(F32)
        low = (local & 63).astype(F32)
        left = jnp.concatenate([hot, hot * high, hot * low], axis=0).astype(BF16)
        right = (iota((2 * CAP, ROWS), 0) == rank + sec * CAP).astype(F32).astype(BF16)
        table = table + lax.dot_general(left, right, NT, preferred_element_type=F32)
    filled = table[:OWNERS]
    value = table[OWNERS : 2 * OWNERS] * 64.0 + table[2 * OWNERS :]
    ids_ref[...] = jnp.where(filled > 0.5, value, -1.0).astype(jnp.int32)


def make_plan(z_low, codes):
    return pl.pallas_call(
        plan_kernel,
        in_specs=[
            pl.BlockSpec(memory_space=pltpu.SMEM),
            pl.BlockSpec(memory_space=pltpu.VMEM),
        ],
        out_shape=(
            jax.ShapeDtypeStruct((OWNERS, 2 * CAP), jnp.int32),
            jax.ShapeDtypeStruct((2, ROWS), jnp.int32),
            jax.ShapeDtypeStruct((2, ROWS), jnp.int32),
        ),
        compiler_params=params(),
        cost_estimate=cost(4 * OWNERS * ROWS * ROWS, 1 << 16),
        name="plan",
    )(z_low, codes)


def columns(row):
    parts = []
    for start in range(0, row.shape[1], 128):
        piece = jnp.broadcast_to(row[:, start : start + 128], (128, 128))
        parts.append(jnp.transpose(piece))
    return jnp.concatenate(parts, axis=0)


def one_hot(cols, width, offset=0):
    lanes = iota(cols.shape, 1)
    parts = [
        (cols == lanes + (offset + start)).astype(F32).astype(BF16)
        for start in range(0, width, 128)
    ]
    return jnp.concatenate(parts, axis=1)


def serve_kernel(ids_ref, table_ref, out_ref):
    picks = one_hot(columns(ids_ref[0]), CODE_ROWS)
    got = jnp.dot(picks, table_ref[0], preferred_element_type=F32)
    out_ref[...] = got.astype(BF16).reshape(out_ref.shape)


def serve(ids, codebooks, sec):
    step = 512
    per = ids.shape[1]
    return pl.pallas_call(
        serve_kernel,
        grid=(ids.size // step,),
        in_specs=[
            pl.BlockSpec((1, 1, step), lambda i: (i, 0, 0)),
            pl.BlockSpec((1, CODE_ROWS, CH), lambda i: (sec, 0, 0)),
        ],
        out_specs=pl.BlockSpec((step // per, per, CH), lambda i: (i, 0, 0)),
        out_shape=jax.ShapeDtypeStruct((PLANE, per, CH), BF16),
        compiler_params=params("arbitrary"),
        cost_estimate=cost(2 * ids.size * CODE_ROWS * CH, 4 << 20),
        name="serve",
    )(ids.reshape(-1, 1, step), codebooks)


def picked(place_row, tables):
    cols = columns(place_row)
    got, start = None, 0
    for table in tables:
        size = table.shape[0] * table.shape[1]
        made = jnp.dot(
            one_hot(cols, size, start),
            table[...].reshape(size, CH),
            preferred_element_type=F32,
        )
        got = made if got is None else got + made
        start += size
    return got


def unpack_kernel(place_ref, *refs):
    refs[-1][...] = picked(place_ref[0], refs[:-1]).astype(BF16)


def unpack(place, tables):
    step = 512
    whole = [pl.BlockSpec(table.shape, lambda i: (0, 0, 0)) for table in tables]
    return pl.pallas_call(
        unpack_kernel,
        grid=(ROWS // step,),
        in_specs=[pl.BlockSpec((1, 1, step), lambda i: (i, 0, 0)), *whole],
        out_specs=pl.BlockSpec((step, CH), lambda i: (i, 0)),
        out_shape=jax.ShapeDtypeStruct((ROWS, CH), BF16),
        compiler_params=params("arbitrary"),
        cost_estimate=cost(2 * ROWS * CODE_ROWS * CH, 3 << 20),
        name="unpack",
    )(place.reshape(ROWS // step, 1, step), *tables)


def conv_kernel(before_ref, own_ref, after_ref, gain_ref, weight_ref, out_ref, normed_ref):
    @pl.when(pl.program_id(0) == 0)
    def _():
        def put(values, start):
            wide = values.astype(F32)
            inverse = lax.rsqrt(jnp.mean(wide * wide, axis=-1, keepdims=True) + 1e-06)
            normed_ref[:, start : start + values.shape[1], :] = (
                wide * inverse * gain_ref[...]
            ).astype(BF16)

        put(own_ref[...], 128)
        put(before_ref[...], 0)
        put(after_ref[...], 384)

    frames = normed_ref.shape[0]
    width = out_ref.shape[-1]
    column = iota((frames * 256, width), 0) & 127
    total = None
    for col in (1, 0, 2):
        part = None
        for row in range(3):
            window = normed_ref[:, row * 128 : row * 128 + 256, :].reshape(frames * 256, CH)
            made = jnp.dot(window, weight_ref[row, col], preferred_element_type=F32)
            part = made if part is None else part + made
        if col == 0:
            part = jnp.where(column == 0, 0.0, pltpu.roll(part, 1, 0))
        elif col == 2:
            part = jnp.where(column == 127, 0.0, pltpu.roll(part, frames * 256 - 1, 0))
        total = part if total is None else total + part
    out_ref[...] = (total / (1.0 + jnp.exp(-total))).astype(BF16).reshape(out_ref.shape)


def convolve(before, own, after, gain, weight):
    width = 256
    frames = own.shape[0]
    whole = lambda rows: pl.BlockSpec((frames, rows, CH), lambda i: (0, 0, 0))
    return pl.pallas_call(
        conv_kernel,
        grid=(CH // width,),
        in_specs=[
            whole(128),
            whole(256),
            whole(128),
            pl.BlockSpec((1, 1, CH), lambda i: (0, 0, 0)),
            pl.BlockSpec((3, 3, CH, width), lambda i: (0, 0, 0, i)),
        ],
        out_specs=pl.BlockSpec((frames, 256, width), lambda i: (0, 0, i)),
        out_shape=jax.ShapeDtypeStruct((frames, 256, CH), BF16),
        scratch_shapes=[pltpu.VMEM((frames, 512, CH), BF16)],
        compiler_params=params("arbitrary"),
        cost_estimate=cost(18 * ROWS * CH * CH, 8 << 20),
        name="conv",
    )(before, own, after, gain.reshape(1, 1, CH), weight)


def pack_into(turned_ref, slot_row, out_ref):
    step = 256
    left = iota((SLABS, HALF, 128), 2) < 64

    def chunk(index, carry):
        hot = (iota((step, ROWS), 0) + index * step == slot_row).astype(F32).astype(BF16)
        block = lax.dot_general(turned_ref[...], hot, NT, preferred_element_type=F32)
        for pair in range(step // 128):
            piece = block[:, pair * 128 : (pair + 1) * 128].reshape(SLABS, CHUNK, 128)
            top, low = piece[:, :HALF], piece[:, HALF:]
            owner = index * (step // CAP) + 2 * pair
            out_ref[:, owner] = jnp.where(left, top, pltpu.roll(low, 64, 2)).astype(BF16)
            out_ref[:, owner + 1] = jnp.where(left, pltpu.roll(top, 64, 2), low).astype(BF16)
        return carry

    lax.fori_loop(0, OWNERS * CAP // step, chunk, 0)


MESSAGE = jax.ShapeDtypeStruct((SLABS, OWNERS, HALF, 128), BF16)


def first_kernel(lat_ref, hid_ref, prev_ref, taps_ref, slot_ref, out_ref, enc_ref, turned_ref):
    taps = [taps_ref[tap : tap + 1, :] for tap in range(3)]
    clips, frames = lat_ref.shape[0], lat_ref.shape[1]
    for clip in range(clips):
        series = [prev_ref[clip, f].astype(F32) for f in range(frames)]
        series += [hid_ref[clip, f].astype(F32) for f in range(frames)]
        for frame in range(frames):
            mixed = taps[0] * series[frame]
            mixed = mixed + taps[1] * series[frame + 1]
            mixed = mixed + taps[2] * series[frame + 2]
            made = (lat_ref[clip, frame].astype(F32) + mixed).astype(BF16)
            start = (clip * frames + frame) * 256
            enc_ref[start : start + 256, :] = made
            turned_ref[:, start : start + 256] = jnp.transpose(made.astype(F32)).astype(BF16)
    pack_into(turned_ref, slot_ref[...], out_ref)


def pack_first(lat, hid, prev, taps, slot):
    return pl.pallas_call(
        first_kernel,
        out_shape=(MESSAGE, jax.ShapeDtypeStruct((ROWS, CH), BF16)),
        scratch_shapes=[pltpu.VMEM((CH, ROWS), BF16)],
        compiler_params=params(),
        cost_estimate=cost(2 * ROWS * CODE_ROWS * CH, 6 << 20),
        name="pack_first",
    )(lat, hid, prev, taps, slot)


def second_kernel(enc_ref, place_ref, slot_ref, *refs):
    out_ref, res_ref, turned_ref = refs[-3:]
    for start in range(0, ROWS, 512):
        quant = picked(place_ref[:, start : start + 512], refs[:-3])
        made = (enc_ref[start : start + 512, :].astype(F32) - quant).astype(BF16)
        res_ref[start : start + 512, :] = made
        turned_ref[:, start : start + 512] = jnp.transpose(made.astype(F32)).astype(BF16)
    pack_into(turned_ref, slot_ref[...], out_ref)


def pack_second(enc, place, slot, tables):
    return pl.pallas_call(
        second_kernel,
        out_shape=(MESSAGE, jax.ShapeDtypeStruct((ROWS, CH), BF16)),
        scratch_shapes=[pltpu.VMEM((CH, ROWS), BF16)],
        compiler_params=params(),
        cost_estimate=cost(4 * ROWS * CODE_ROWS * CH, 6 << 20),
        name="pack_second",
    )(enc, place, slot, *tables)


def counts_kernel(ids_ref, ema_ref, keep_ref, out_ref, acc_ref):
    step = pl.program_id(0)

    @pl.when(step == 0)
    def _():
        acc_ref[...] = jnp.zeros_like(acc_ref)

    groups = CODE_ROWS // CH
    for sec in range(2):
        hots, rows = [], []
        for pair in range(ids_ref.shape[2]):
            code = ids_ref[sec, 0, pair : pair + 1, :]
            hots.append((iota((CH, 128), 0) == (code & (CH - 1))).astype(F32).astype(BF16))
            rows.append((iota((8, 128), 0) == (code >> 9)).astype(F32).astype(BF16))
        acc_ref[sec] += lax.dot_general(
            jnp.concatenate(rows, axis=1),
            jnp.concatenate(hots, axis=1),
            NT,
            preferred_element_type=F32,
        )

    @pl.when(step == pl.num_programs(0) - 1)
    def _():
        for sec in range(2):
            keep = keep_ref[sec]
            for g in range(groups):
                span = slice(g * CH, (g + 1) * CH)
                out_ref[sec : sec + 1, span] = (
                    keep * ema_ref[sec : sec + 1, span]
                    + (1.0 - keep) * acc_ref[sec, g : g + 1, :]
                )


def new_counts(ids, ema_counts, decay):
    steps = ids.shape[1]
    whole = pl.BlockSpec((2, CODE_ROWS), lambda i: (0, 0))
    return pl.pallas_call(
        counts_kernel,
        grid=(steps,),
        in_specs=[
            pl.BlockSpec((2, 1, *ids.shape[2:]), lambda i: (0, i, 0, 0)),
            whole,
            pl.BlockSpec(memory_space=pltpu.SMEM),
        ],
        out_specs=whole,
        out_shape=jax.ShapeDtypeStruct((2, CODE_ROWS), F32),
        scratch_shapes=[pltpu.VMEM((2, 8, CH), F32)],
        compiler_params=params("arbitrary"),
        cost_estimate=cost(4 * 128 * CH * 256 * CAP, 1 << 18),
        name="counts",
    )(ids, ema_counts, decay)


def sums_kernel(sec, got_ref, ids_ref, ema_ref, decay_ref, *rest):
    out_ref, acc_ref = rest[-2:]
    step = pl.program_id(0)
    left = iota((HALF, 128), 1) < 64
    groups = CODE_ROWS // CH
    hots, wides = [], []
    for pair in range(got_ref.shape[0] // 2):
        code = ids_ref[0, 0, pair : pair + 1, :]
        group = code >> 9
        hots.append((iota((CH, 128), 0) == (code & (CH - 1))).astype(F32).astype(BF16))
        one = got_ref[2 * pair].astype(F32)
        two = got_ref[2 * pair + 1].astype(F32)
        block = jnp.concatenate(
            [
                jnp.where(left, one, pltpu.roll(two, 64, 1)),
                jnp.where(left, pltpu.roll(one, 64, 1), two),
            ],
            axis=0,
        )
        rows = [jnp.where(group == g, block, 0.0) for g in range(groups)]
        wides.append(jnp.concatenate(rows, axis=0).astype(BF16))
    hot = jnp.concatenate(hots, axis=1)
    wide = jnp.concatenate(wides, axis=1)
    made = lax.dot_general(wide, hot, NT, preferred_element_type=F32)

    @pl.when(step == 0)
    def _():
        acc_ref[...] = made

    @pl.when(step != 0)
    def _():
        acc_ref[...] += made

    @pl.when(step == pl.num_programs(0) - 1)
    def _():
        keep = decay_ref[sec]
        for g in range(groups):
            span = slice(g * CH, (g + 1) * CH)
            out_ref[0, :, span] = keep * ema_ref[0, :, span] + (1.0 - keep) * acc_ref[
                g * CHUNK : (g + 1) * CHUNK, :
            ]


def sums(sec, got, ids, ema, decay, earlier=None):
    sources = 2 * ids.shape[2]
    block = pl.BlockSpec((1, CHUNK, CODE_ROWS), lambda i: (sec, 0, 0))
    in_specs = [
        pl.BlockSpec((sources, HALF, 128), lambda i: (i, 0, 0)),
        pl.BlockSpec((1, 1, *ids.shape[2:]), lambda i: (sec, i, 0, 0)),
        block,
        pl.BlockSpec(memory_space=pltpu.SMEM),
    ]
    args = [got, ids, ema, decay]
    aliases = {}
    if earlier is not None:
        in_specs.append(pl.BlockSpec(memory_space=pl.ANY))
        args.append(earlier)
        aliases = {4: 0}
    return pl.pallas_call(
        functools.partial(sums_kernel, sec),
        grid=(got.shape[0] // sources,),
        in_specs=in_specs,
        out_specs=block,
        out_shape=jax.ShapeDtypeStruct((2, CHUNK, CODE_ROWS), F32),
        scratch_shapes=[pltpu.VMEM((CODE_ROWS // CH * CHUNK, CH), F32)],
        input_output_aliases=aliases,
        compiler_params=params("arbitrary"),
        cost_estimate=cost(2 * 256 * CH * 256 * CAP, 4 << 20),
        name="sums",
    )(*args)


def device(y, z, inner):
    return (y * 2 + z // 4) * OWNERS + (z % 4) * PLANE + inner


def along_z(x, steps):
    pairs = [
        (device(y, z, inner), device(y, (z + steps) % 8, inner))
        for y in range(4)
        for z in range(8)
        for inner in range(PLANE)
    ]
    return lax.ppermute(x, BOTH, pairs)


def in_plane(x):
    groups = [list(range(z * PLANE, (z + 1) * PLANE)) for z in range(4)]
    return lax.all_to_all(x, "height", 0, 0, axis_index_groups=groups, tiled=True)


def spread(served):
    got = in_plane(served)
    ahead, behind = got[:, CAP : 2 * CAP], got[:, 2 * CAP : 3 * CAP]
    far_ahead, far_behind = got[:, 3 * CAP : 3 * CAP + HALF], got[:, 3 * CAP + HALF :]
    moved = (along_z(ahead, 1), along_z(behind, -1), along_z(far_behind, -2), along_z(far_ahead, 2))
    return (got[:, :CAP], *moved)


def sent_to_owners(message):
    return lax.all_to_all(message.reshape(-1, HALF, 128), BOTH, 0, 0, tiled=True)


def block(
    latents,
    norm_gain,
    spatial_weight,
    temporal_weight,
    codebooks,
    ema_counts,
    ema_sums,
    decay,
    codes_first,
    codes_second,
):
    tm, height = lax.axis_index("tm"), lax.axis_index("height")
    up = [(i, i + 1) for i in range(OWNERS - 1)]
    down = [(i + 1, i) for i in range(OWNERS - 1)]
    before = lax.ppermute(latents[:, :, 1], "height", up).reshape(4, 128, CH)
    after = lax.ppermute(latents[:, :, 0], "height", down).reshape(4, 128, CH)

    codes = jnp.stack([codes_first.reshape(ROWS), codes_second.reshape(ROWS)])
    z_low = height // PLANE
    ids, slot, place = make_plan(z_low.reshape(1), codes)
    sent = jnp.broadcast_to(ids[None], (2, OWNERS, 2 * CAP)).reshape(-1, 2 * CAP)
    sheets = [list(range(y * 2 * OWNERS, (y + 1) * 2 * OWNERS)) for y in range(4)]
    asked = lax.all_to_all(sent, BOTH, 0, 0, axis_index_groups=sheets, tiled=True)

    own = latents.reshape(4, 256, CH)
    hidden = convolve(before, own, after, norm_gain, spatial_weight)
    previous = lax.ppermute(hidden, "tm", [(i, i + 1) for i in range(SLABS - 1)])
    asked, hidden = lax.optimization_barrier((asked, hidden))

    rings = [list(range(start, SLABS, 2)) for start in range(2)]
    known = lax.all_gather(asked, "tm", axis_index_groups=rings, tiled=True)
    by_z = asked.reshape(8, PLANE, 2 * CAP)
    here = (tm & 1) * 4 + z_low
    wanted = {
        step: lax.dynamic_index_in_dim(by_z, (here + step) & 7, 0, keepdims=False)
        for step in (0, 1, -1, 2, -2)
    }
    answers = []
    for sec in range(2):
        start = sec * CAP
        rows = jnp.concatenate(
            [
                wanted[0][:, start : start + CAP],
                wanted[1][:, start : start + CAP],
                wanted[-1][:, start : start + CAP],
                wanted[2][:, start + HALF : start + CAP],
                wanted[-2][:, start : start + HALF],
            ],
            axis=1,
        )
        served = serve(rows, codebooks, sec)
        answers.append(spread(served))

    clip_form = lambda x: x.reshape(2, 2, 256, CH)
    first_out, encoded = pack_first(
        clip_form(latents), clip_form(hidden), clip_form(previous), temporal_weight, slot[:1]
    )
    first_in = sent_to_owners(first_out)
    second_out, residual = pack_second(encoded, place[:1], slot[1:], answers[0])
    second_in = sent_to_owners(second_out)

    second_quant = unpack(place[1], answers[1])
    leftover = residual.astype(F32) - second_quant.astype(F32)
    error = jnp.mean(leftover * leftover, axis=-1).reshape(codes_first.shape)

    turned_ema = jnp.swapaxes(ema_sums, 1, 2)
    pair_ids = jnp.stack(
        [known[:, sec * CAP : (sec + 1) * CAP].reshape(8, 16, 128) for sec in range(2)]
    )
    ema_counts_new = new_counts(pair_ids, ema_counts, decay)
    partial = sums(0, first_in, pair_ids, turned_ema, decay)
    done = sums(1, second_in, pair_ids, turned_ema, decay, partial)
    ema_sums_new = jnp.swapaxes(done, 1, 2)
    return (ema_counts_new, ema_sums_new, error)


def solution(mesh):
    return jax.shard_map(
        block,
        mesh=mesh,
        in_specs=(
            P(None, "tm", "height", None, None),
            P(),
            P(),
            P(),
            P(None, "height", None),
            P(None, "height"),
            P(None, "height", "tm"),
            P(),
            P(None, "tm", "height", None),
            P(None, "tm", "height", None),
        ),
        out_specs=(P(None, "height"), P(None, "height", "tm"), P(None, "tm", "height", None)),
        check_vma=False,
    )
```

```python
import functools

import jax
import jax.numpy as jnp
from jax import lax
from jax.experimental import pallas as pl
from jax.experimental.pallas import tpu as pltpu
from jax.sharding import PartitionSpec as P


BOTH = ("tm", "height")
OWNERS = 32
SLABS = 8
CAP = 64
HALF = CAP // 2
PLANE = 8
ROWS = 1024
CH = 512
CHUNK = CH // SLABS
CODE_ROWS = 2048
VMEM_LIMIT = 56 * 1024 * 1024
NT = (((1,), (1,)), ((), ()))
F32 = jnp.float32
BF16 = jnp.bfloat16


def iota(shape, dim):
    return lax.broadcasted_iota(jnp.int32, shape, dim)


def params(*semantics):
    return pltpu.CompilerParams(
        vmem_limit_bytes=VMEM_LIMIT, dimension_semantics=semantics or None
    )


def cost(flops, moved):
    return pl.CostEstimate(flops=flops, transcendentals=0, bytes_accessed=moved)


def plan_kernel(z_ref, codes_ref, ids_ref, slot_ref, place_ref):
    tri = (iota((ROWS, ROWS), 0) < iota((ROWS, ROWS), 1)).astype(F32).astype(BF16)
    table = jnp.zeros((3 * OWNERS, 2 * CAP), F32)
    for sec in range(2):
        code = codes_ref[sec : sec + 1, :]
        owner = code >> 11
        local = code & (CODE_ROWS - 1)
        hot = (iota((OWNERS, ROWS), 0) == owner).astype(F32)
        ahead = jnp.dot(hot.astype(BF16), tri, preferred_element_type=F32)
        rank = jnp.sum(hot * ahead, axis=0, keepdims=True).astype(jnp.int32)
        slot_ref[sec : sec + 1, :] = owner * CAP + rank
        away = ((owner >> 3) - z_ref[0]) & 3
        inner = (owner & 7) ^ (z_ref[1] if sec else 0)
        full = jnp.where(away == 0, 0, jnp.where(away == 3, PLANE * CAP, 2 * PLANE * CAP))
        split = 3 * PLANE * CAP + (rank >> 5) * (PLANE * HALF) + inner * HALF + (rank & (HALF - 1))
        place_ref[sec : sec + 1, :] = jnp.where(away == 2, split, full + inner * CAP + rank)
        high = (local >> 6).astype(F32)
        low = (local & 63).astype(F32)
        left = jnp.concatenate([hot, hot * high, hot * low], axis=0).astype(BF16)
        right = (iota((2 * CAP, ROWS), 0) == rank + sec * CAP).astype(F32).astype(BF16)
        table = table + lax.dot_general(left, right, NT, preferred_element_type=F32)
    filled = table[:OWNERS]
    value = table[OWNERS : 2 * OWNERS] * 64.0 + table[2 * OWNERS :]
    ids_ref[...] = jnp.where(filled > 0.5, value, -1.0).astype(jnp.int32)


def make_plan(z_low, codes):
    return pl.pallas_call(
        plan_kernel,
        in_specs=[
            pl.BlockSpec(memory_space=pltpu.SMEM),
            pl.BlockSpec(memory_space=pltpu.VMEM),
        ],
        out_shape=(
            jax.ShapeDtypeStruct((OWNERS, 2 * CAP), jnp.int32),
            jax.ShapeDtypeStruct((2, ROWS), jnp.int32),
            jax.ShapeDtypeStruct((2, ROWS), jnp.int32),
        ),
        compiler_params=params(),
        cost_estimate=cost(4 * OWNERS * ROWS * ROWS, 1 << 16),
        name="plan",
    )(z_low, codes)


def columns(row):
    parts = []
    for start in range(0, row.shape[1], 128):
        piece = jnp.broadcast_to(row[:, start : start + 128], (128, 128))
        parts.append(jnp.transpose(piece))
    return jnp.concatenate(parts, axis=0)


def one_hot(cols, width, offset=0):
    lanes = iota(cols.shape, 1)
    parts = [
        (cols == lanes + (offset + start)).astype(F32).astype(BF16)
        for start in range(0, width, 128)
    ]
    return jnp.concatenate(parts, axis=1)


def serve_kernel(ids_ref, table_ref, out_ref):
    picks = one_hot(columns(ids_ref[0]), CODE_ROWS)
    got = jnp.dot(picks, table_ref[0], preferred_element_type=F32)
    out_ref[...] = got.astype(BF16).reshape(out_ref.shape)


def serve(ids, codebooks, sec):
    step = 512
    per = ids.shape[1]
    return pl.pallas_call(
        serve_kernel,
        grid=(ids.size // step,),
        in_specs=[
            pl.BlockSpec((1, 1, step), lambda i: (i, 0, 0)),
            pl.BlockSpec((1, CODE_ROWS, CH), lambda i: (sec, 0, 0)),
        ],
        out_specs=pl.BlockSpec((step // per, per, CH), lambda i: (i, 0, 0)),
        out_shape=jax.ShapeDtypeStruct((PLANE, per, CH), BF16),
        compiler_params=params("arbitrary"),
        cost_estimate=cost(2 * ids.size * CODE_ROWS * CH, 4 << 20),
        name="serve",
    )(ids.reshape(-1, 1, step), codebooks)


def picked(place_row, tables):
    cols = columns(place_row)
    got, start = None, 0
    for table in tables:
        size = table.shape[0] * table.shape[1]
        made = jnp.dot(
            one_hot(cols, size, start),
            table[...].reshape(size, CH),
            preferred_element_type=F32,
        )
        got = made if got is None else got + made
        start += size
    return got


def unpack_kernel(place_ref, *refs):
    refs[-1][...] = picked(place_ref[0], refs[:-1]).astype(BF16)


def unpack(place, tables):
    step = 512
    whole = [pl.BlockSpec(table.shape, lambda i: (0, 0, 0)) for table in tables]
    return pl.pallas_call(
        unpack_kernel,
        grid=(ROWS // step,),
        in_specs=[pl.BlockSpec((1, 1, step), lambda i: (i, 0, 0)), *whole],
        out_specs=pl.BlockSpec((step, CH), lambda i: (i, 0)),
        out_shape=jax.ShapeDtypeStruct((ROWS, CH), BF16),
        compiler_params=params("arbitrary"),
        cost_estimate=cost(2 * ROWS * CODE_ROWS * CH, 3 << 20),
        name="unpack",
    )(place.reshape(ROWS // step, 1, step), *tables)


def conv_kernel(before_ref, own_ref, after_ref, gain_ref, weight_ref, out_ref, normed_ref):
    @pl.when(pl.program_id(0) == 0)
    def _():
        def put(values, start):
            wide = values.astype(F32)
            inverse = lax.rsqrt(jnp.mean(wide * wide, axis=-1, keepdims=True) + 1e-06)
            normed_ref[:, start : start + values.shape[1], :] = (
                wide * inverse * gain_ref[...]
            ).astype(BF16)

        put(own_ref[...], 128)
        put(before_ref[...], 0)
        put(after_ref[...], 384)

    frames = normed_ref.shape[0]
    width = out_ref.shape[-1]
    column = iota((frames * 256, width), 0) & 127
    total = None
    for col in (1, 0, 2):
        part = None
        for row in range(3):
            window = normed_ref[:, row * 128 : row * 128 + 256, :].reshape(frames * 256, CH)
            made = jnp.dot(window, weight_ref[row, col], preferred_element_type=F32)
            part = made if part is None else part + made
        if col == 0:
            part = jnp.where(column == 0, 0.0, pltpu.roll(part, 1, 0))
        elif col == 2:
            part = jnp.where(column == 127, 0.0, pltpu.roll(part, frames * 256 - 1, 0))
        total = part if total is None else total + part
    out_ref[...] = (total / (1.0 + jnp.exp(-total))).astype(BF16).reshape(out_ref.shape)


def convolve(before, own, after, gain, weight):
    width = 256
    frames = own.shape[0]
    whole = lambda rows: pl.BlockSpec((frames, rows, CH), lambda i: (0, 0, 0))
    return pl.pallas_call(
        conv_kernel,
        grid=(CH // width,),
        in_specs=[
            whole(128),
            whole(256),
            whole(128),
            pl.BlockSpec((1, 1, CH), lambda i: (0, 0, 0)),
            pl.BlockSpec((3, 3, CH, width), lambda i: (0, 0, 0, i)),
        ],
        out_specs=pl.BlockSpec((frames, 256, width), lambda i: (0, 0, i)),
        out_shape=jax.ShapeDtypeStruct((frames, 256, CH), BF16),
        scratch_shapes=[pltpu.VMEM((frames, 512, CH), BF16)],
        compiler_params=params("arbitrary"),
        cost_estimate=cost(18 * ROWS * CH * CH, 8 << 20),
        name="conv",
    )(before, own, after, gain.reshape(1, 1, CH), weight)


def pack_into(turned_ref, slot_row, out_ref):
    step = 256
    left = iota((SLABS, HALF, 128), 2) < 64

    def chunk(index, carry):
        hot = (iota((step, ROWS), 0) + index * step == slot_row).astype(F32).astype(BF16)
        block = lax.dot_general(turned_ref[...], hot, NT, preferred_element_type=F32)
        for pair in range(step // 128):
            piece = block[:, pair * 128 : (pair + 1) * 128].reshape(SLABS, CHUNK, 128)
            top, low = piece[:, :HALF], piece[:, HALF:]
            owner = index * (step // CAP) + 2 * pair
            out_ref[:, owner] = jnp.where(left, top, pltpu.roll(low, 64, 2)).astype(BF16)
            out_ref[:, owner + 1] = jnp.where(left, pltpu.roll(top, 64, 2), low).astype(BF16)
        return carry

    lax.fori_loop(0, OWNERS * CAP // step, chunk, 0)


MESSAGE = jax.ShapeDtypeStruct((SLABS, OWNERS, HALF, 128), BF16)


def first_kernel(lat_ref, hid_ref, prev_ref, taps_ref, slot_ref, out_ref, enc_ref, turned_ref):
    taps = [taps_ref[tap : tap + 1, :] for tap in range(3)]
    clips, frames = lat_ref.shape[0], lat_ref.shape[1]
    for clip in range(clips):
        series = [prev_ref[clip, f].astype(F32) for f in range(frames)]
        series += [hid_ref[clip, f].astype(F32) for f in range(frames)]
        for frame in range(frames):
            mixed = taps[0] * series[frame]
            mixed = mixed + taps[1] * series[frame + 1]
            mixed = mixed + taps[2] * series[frame + 2]
            made = (lat_ref[clip, frame].astype(F32) + mixed).astype(BF16)
            start = (clip * frames + frame) * 256
            enc_ref[start : start + 256, :] = made
            turned_ref[:, start : start + 256] = jnp.transpose(made.astype(F32)).astype(BF16)
    pack_into(turned_ref, slot_ref[...], out_ref)


def pack_first(lat, hid, prev, taps, slot):
    return pl.pallas_call(
        first_kernel,
        out_shape=(MESSAGE, jax.ShapeDtypeStruct((ROWS, CH), BF16)),
        scratch_shapes=[pltpu.VMEM((CH, ROWS), BF16)],
        compiler_params=params(),
        cost_estimate=cost(2 * ROWS * CODE_ROWS * CH, 6 << 20),
        name="pack_first",
    )(lat, hid, prev, taps, slot)


def second_kernel(enc_ref, place_ref, slot_ref, *refs):
    out_ref, res_ref, turned_ref = refs[-3:]
    for start in range(0, ROWS, 512):
        quant = picked(place_ref[:, start : start + 512], refs[:-3])
        made = (enc_ref[start : start + 512, :].astype(F32) - quant).astype(BF16)
        res_ref[start : start + 512, :] = made
        turned_ref[:, start : start + 512] = jnp.transpose(made.astype(F32)).astype(BF16)
    pack_into(turned_ref, slot_ref[...], out_ref)


def pack_second(enc, place, slot, tables):
    return pl.pallas_call(
        second_kernel,
        out_shape=(MESSAGE, jax.ShapeDtypeStruct((ROWS, CH), BF16)),
        scratch_shapes=[pltpu.VMEM((CH, ROWS), BF16)],
        compiler_params=params(),
        cost_estimate=cost(4 * ROWS * CODE_ROWS * CH, 6 << 20),
        name="pack_second",
    )(enc, place, slot, *tables)


def counts_kernel(ids_ref, ema_ref, keep_ref, out_ref, acc_ref):
    step = pl.program_id(0)

    @pl.when(step == 0)
    def _():
        acc_ref[...] = jnp.zeros_like(acc_ref)

    groups = CODE_ROWS // CH
    for sec in range(2):
        hots, rows = [], []
        for pair in range(ids_ref.shape[2]):
            code = ids_ref[sec, 0, pair : pair + 1, :]
            hots.append((iota((CH, 128), 0) == (code & (CH - 1))).astype(F32).astype(BF16))
            rows.append((iota((8, 128), 0) == (code >> 9)).astype(F32).astype(BF16))
        acc_ref[sec] += lax.dot_general(
            jnp.concatenate(rows, axis=1),
            jnp.concatenate(hots, axis=1),
            NT,
            preferred_element_type=F32,
        )

    @pl.when(step == pl.num_programs(0) - 1)
    def _():
        for sec in range(2):
            keep = keep_ref[sec]
            for g in range(groups):
                span = slice(g * CH, (g + 1) * CH)
                out_ref[sec : sec + 1, span] = (
                    keep * ema_ref[sec : sec + 1, span]
                    + (1.0 - keep) * acc_ref[sec, g : g + 1, :]
                )


def new_counts(ids, ema_counts, decay):
    steps = ids.shape[1]
    whole = pl.BlockSpec((2, CODE_ROWS), lambda i: (0, 0))
    return pl.pallas_call(
        counts_kernel,
        grid=(steps,),
        in_specs=[
            pl.BlockSpec((2, 1, *ids.shape[2:]), lambda i: (0, i, 0, 0)),
            whole,
            pl.BlockSpec(memory_space=pltpu.SMEM),
        ],
        out_specs=whole,
        out_shape=jax.ShapeDtypeStruct((2, CODE_ROWS), F32),
        scratch_shapes=[pltpu.VMEM((2, 8, CH), F32)],
        compiler_params=params("arbitrary"),
        cost_estimate=cost(4 * 128 * CH * 256 * CAP, 1 << 18),
        name="counts",
    )(ids, ema_counts, decay)


def sums_kernel(sec, got_ref, ids_ref, ema_ref, decay_ref, *rest):
    out_ref, acc_ref = rest[-2:]
    step = pl.program_id(0)
    left = iota((HALF, 128), 1) < 64
    groups = CODE_ROWS // CH
    hots, wides = [], []
    for pair in range(got_ref.shape[0] // 2):
        code = ids_ref[0, 0, pair : pair + 1, :]
        group = code >> 9
        hots.append((iota((CH, 128), 0) == (code & (CH - 1))).astype(F32).astype(BF16))
        one = got_ref[2 * pair].astype(F32)
        two = got_ref[2 * pair + 1].astype(F32)
        block = jnp.concatenate(
            [
                jnp.where(left, one, pltpu.roll(two, 64, 1)),
                jnp.where(left, pltpu.roll(one, 64, 1), two),
            ],
            axis=0,
        )
        rows = [jnp.where(group == g, block, 0.0) for g in range(groups)]
        wides.append(jnp.concatenate(rows, axis=0).astype(BF16))
    hot = jnp.concatenate(hots, axis=1)
    wide = jnp.concatenate(wides, axis=1)
    made = lax.dot_general(wide, hot, NT, preferred_element_type=F32)

    @pl.when(step == 0)
    def _():
        acc_ref[...] = made

    @pl.when(step != 0)
    def _():
        acc_ref[...] += made

    @pl.when(step == pl.num_programs(0) - 1)
    def _():
        keep = decay_ref[sec]
        for g in range(groups):
            span = slice(g * CH, (g + 1) * CH)
            out_ref[0, :, span] = keep * ema_ref[0, :, span] + (1.0 - keep) * acc_ref[
                g * CHUNK : (g + 1) * CHUNK, :
            ]


def sums(sec, got, ids, ema, decay, earlier=None):
    sources = 2 * ids.shape[2]
    block = pl.BlockSpec((1, CHUNK, CODE_ROWS), lambda i: (sec, 0, 0))
    in_specs = [
        pl.BlockSpec((sources, HALF, 128), lambda i: (i, 0, 0)),
        pl.BlockSpec((1, 1, *ids.shape[2:]), lambda i: (sec, i, 0, 0)),
        block,
        pl.BlockSpec(memory_space=pltpu.SMEM),
    ]
    args = [got, ids, ema, decay]
    aliases = {}
    if earlier is not None:
        in_specs.append(pl.BlockSpec(memory_space=pl.ANY))
        args.append(earlier)
        aliases = {4: 0}
    return pl.pallas_call(
        functools.partial(sums_kernel, sec),
        grid=(got.shape[0] // sources,),
        in_specs=in_specs,
        out_specs=block,
        out_shape=jax.ShapeDtypeStruct((2, CHUNK, CODE_ROWS), F32),
        scratch_shapes=[pltpu.VMEM((CODE_ROWS // CH * CHUNK, CH), F32)],
        input_output_aliases=aliases,
        compiler_params=params("arbitrary"),
        cost_estimate=cost(2 * 256 * CH * 256 * CAP, 4 << 20),
        name="sums",
    )(*args)


def device(y, z, inner):
    return (y * 2 + z // 4) * OWNERS + (z % 4) * PLANE + inner


def along_z(x, steps):
    pairs = [
        (device(y, z, inner), device(y, (z + steps) % 8, inner))
        for y in range(4)
        for z in range(8)
        for inner in range(PLANE)
    ]
    return lax.ppermute(x, BOTH, pairs)


def in_plane(x):
    groups = [list(range(z * PLANE, (z + 1) * PLANE)) for z in range(4)]
    return lax.all_to_all(x, "height", 0, 0, axis_index_groups=groups, tiled=True)


def in_plane_apart(x, inner):
    parts = [lax.dynamic_slice_in_dim(x, inner, 1, 0)]
    for k in range(1, PLANE):
        pairs = [(z + i, z + (i ^ k)) for z in range(0, OWNERS, PLANE) for i in range(PLANE)]
        piece = lax.dynamic_slice_in_dim(x, inner ^ k, 1, 0)
        parts.append(lax.ppermute(piece, "height", pairs))
    return parts


def spread(served, sec, inner):
    got = in_plane(served) if sec == 0 else in_plane_apart(served, inner)
    if sec == 1:
        got = jnp.concatenate(got, axis=0)
    ahead, behind = got[:, CAP : 2 * CAP], got[:, 2 * CAP : 3 * CAP]
    far_ahead, far_behind = got[:, 3 * CAP : 3 * CAP + HALF], got[:, 3 * CAP + HALF :]
    moved = (along_z(ahead, 1), along_z(behind, -1), along_z(far_behind, -2), along_z(far_ahead, 2))
    return (got[:, :CAP], *moved)


def sent_to_owners(message):
    return lax.all_to_all(message.reshape(-1, HALF, 128), BOTH, 0, 0, tiled=True)


def block(
    latents,
    norm_gain,
    spatial_weight,
    temporal_weight,
    codebooks,
    ema_counts,
    ema_sums,
    decay,
    codes_first,
    codes_second,
):
    tm, height = lax.axis_index("tm"), lax.axis_index("height")
    up = [(i, i + 1) for i in range(OWNERS - 1)]
    down = [(i + 1, i) for i in range(OWNERS - 1)]
    before = lax.ppermute(latents[:, :, 1], "height", up).reshape(4, 128, CH)
    after = lax.ppermute(latents[:, :, 0], "height", down).reshape(4, 128, CH)

    codes = jnp.stack([codes_first.reshape(ROWS), codes_second.reshape(ROWS)])
    z_low, inner = height // PLANE, height % PLANE
    ids, slot, place = make_plan(jnp.stack([z_low, inner]), codes)
    sent = jnp.broadcast_to(ids[None], (2, OWNERS, 2 * CAP)).reshape(-1, 2 * CAP)
    sheets = [list(range(y * 2 * OWNERS, (y + 1) * 2 * OWNERS)) for y in range(4)]
    asked = lax.all_to_all(sent, BOTH, 0, 0, axis_index_groups=sheets, tiled=True)

    own = latents.reshape(4, 256, CH)
    hidden = convolve(before, own, after, norm_gain, spatial_weight)
    previous = lax.ppermute(hidden, "tm", [(i, i + 1) for i in range(SLABS - 1)])
    asked, hidden = lax.optimization_barrier((asked, hidden))

    rings = [list(range(start, SLABS, 2)) for start in range(2)]
    known = lax.all_gather(asked, "tm", axis_index_groups=rings, tiled=True)
    by_z = asked.reshape(8, PLANE, 2 * CAP)
    here = (tm & 1) * 4 + z_low
    wanted = {
        step: lax.dynamic_index_in_dim(by_z, (here + step) & 7, 0, keepdims=False)
        for step in (0, 1, -1, 2, -2)
    }
    answers = []
    for sec in range(2):
        start = sec * CAP
        rows = jnp.concatenate(
            [
                wanted[0][:, start : start + CAP],
                wanted[1][:, start : start + CAP],
                wanted[-1][:, start : start + CAP],
                wanted[2][:, start + HALF : start + CAP],
                wanted[-2][:, start : start + HALF],
            ],
            axis=1,
        )
        served = serve(rows, codebooks, sec)
        answers.append(spread(served, sec, inner))

    clip_form = lambda x: x.reshape(2, 2, 256, CH)
    first_out, encoded = pack_first(
        clip_form(latents), clip_form(hidden), clip_form(previous), temporal_weight, slot[:1]
    )
    first_in = sent_to_owners(first_out)
    second_out, residual = pack_second(encoded, place[:1], slot[1:], answers[0])
    second_in = sent_to_owners(second_out)

    second_quant = unpack(place[1], answers[1])
    leftover = residual.astype(F32) - second_quant.astype(F32)
    error = jnp.mean(leftover * leftover, axis=-1).reshape(codes_first.shape)

    turned_ema = jnp.swapaxes(ema_sums, 1, 2)
    pair_ids = jnp.stack(
        [known[:, sec * CAP : (sec + 1) * CAP].reshape(8, 16, 128) for sec in range(2)]
    )
    ema_counts_new = new_counts(pair_ids, ema_counts, decay)
    partial = sums(0, first_in, pair_ids, turned_ema, decay)
    done = sums(1, second_in, pair_ids, turned_ema, decay, partial)
    ema_sums_new = jnp.swapaxes(done, 1, 2)
    return (ema_counts_new, ema_sums_new, error)


def solution(mesh):
    return jax.shard_map(
        block,
        mesh=mesh,
        in_specs=(
            P(None, "tm", "height", None, None),
            P(),
            P(),
            P(),
            P(None, "height", None),
            P(None, "height"),
            P(None, "height", "tm"),
            P(),
            P(None, "tm", "height", None),
            P(None, "tm", "height", None),
        ),
        out_specs=(P(None, "height"), P(None, "height", "tm"), P(None, "tm", "height", None)),
        check_vma=False,
    )
```
